32 devices in a mesh: seq: 8 (over z, x), head: 4 (over y, core).
Axes of the slice: x: 2, y: 2, z: 4, core: 2. Of those that a mesh axis runs over, the one named last changes fastest.
Arguments:
- hidden: bfloat16 [2048, 4096], P(('seq', 'head')), may hold values from -90 to 90
- block_order: int32 [16], replicated, may hold values from 0 to 15, as said below
- segment_ids: int32 [2048], replicated, may hold values from 0 to 3, never falling along the last dimension, each value on 1 to 1024 neighbouring positions
- w_query: bfloat16 [4096, 4096], P(None, 'head'), may hold values from -0.09375 to 0.09375
- key_weight: bfloat16 [4096, 1024], P(None, 'head'), may hold values from -0.09375 to 0.09375
- value_weight: bfloat16 [4096, 1024], P(None, 'head'), may hold values from -0.09375 to 0.09375
- w_out: bfloat16 [4096, 4096], P('head'), may hold values from -0.09375 to 0.09375
Outputs:
- layer_out: bfloat16 [2048, 4096], P(('seq', 'head'))
The draws below stay inside these ranges and needn't reach their ends.
Inputs may be any that keep to these rules, and one draw needn't show every extreme that they name: `block_order`: for each d, entries 2d and 2d+1 are two block numbers that sum to 15; every block number occurs once.
All inputs are finite; a program needn't handle non-finite values.
Results may differ from the reference program's by a relative error of at most 0.018.
The reference program's roundings to bfloat16 on the way (of `attended`) count: a program that leaves them out, or rounds other values in their place, can miss the bound.
Values may be sent and summed in bfloat16 or wider, within the bound.
No kernel may reach another device: no remote copies, remote signals or barrier semaphores. Data moves between devices by JAX's collectives and lax.ppermute only.
A program may use at most 64 MiB of HBM per device.

```python
import math
import jax
import jax.numpy as jnp
import numpy as np
from jax import lax

MODEL_WIDTH = 4096
QUERY_HEADS = 32
KEY_VALUE_HEADS = 8
HEAD_SIZE = 128
TOKENS = 2048
BLK = 128
NBLK = 16
N_HEAD = 4


def draw_hidden(key, part):
    first_key = jax.random.fold_in(key, 0)
    return jnp.clip(jax.random.normal(first_key, (TOKENS, MODEL_WIDTH), jnp.float32), -6.0, 6.0).astype(jnp.bfloat16)


def draw_block_order(key, part):
    first_key, second_key = jax.random.split(jax.random.fold_in(key, 7))
    pairs = NBLK // 2
    shuffled = jax.random.permutation(first_key, pairs).astype(jnp.int32)
    flipped = jax.random.randint(second_key, (pairs,), 0, 2)
    earlier = jnp.where(flipped == 1, shuffled, NBLK - 1 - shuffled)
    later = NBLK - 1 - earlier
    return jnp.stack([earlier, later], axis=1).reshape(NBLK).astype(jnp.int32)


def steps_of(rng, shape, cuts, low, top_value):
    def one(axis_at, shards_of):
        draws = jax.random.uniform(jax.random.fold_in(jax.random.fold_in(rng, 6), axis_at), (shards_of,), jnp.float32, low / len(cuts), top_value / len(cuts))
        return jnp.repeat(jnp.exp(draws), shape[axis_at] // shards_of).reshape((-1,) + (1,) * (len(shape) - axis_at - 1))

    gain = one(*cuts[0])
    for cut in cuts[1:]:
        gain = gain * one(*cut)
    return gain


def length_profile(amount, total, most, slope):
    weights = [(1 << 20) // math.isqrt(rank ** slope) + 1 for rank in range(2, amount + 1)]
    surplus, given = total - most - (amount - 1), [1] * (amount - 1)
    while surplus > 0:
        free = [i for i in range(amount - 1) if given[i] < most]
        pool, left = sum([weights[i] for i in free]), surplus
        for i in free:
            addition = min(most - given[i], max(1, left * weights[i] // pool), surplus)
            given[i] = given[i] + addition
            surplus = surplus - addition
    return np.array([most] + given)


def ragged(own_key, amount, total, limit, slope):
    if amount == 2:
        one = jax.random.randint(own_key, (), max(1, total - limit), min(limit, total - 1) + 1)
        return jnp.stack([one, total - one])
    tallies = jnp.asarray(length_profile(amount, total, limit, slope), jnp.int32)
    pairs = (amount - 1) // 2
    source_of, receiver = tallies[1:1 + 2 * pairs:2], tallies[2:2 + 2 * pairs:2]
    margin = jnp.minimum(source_of - 1, limit - receiver)
    passed = jax.random.randint(jax.random.fold_in(own_key, 1), (pairs,), 0, 1 << 20) % (margin + 1)
    tallies = tallies.at[1:1 + 2 * pairs:2].set(source_of - passed).at[2:2 + 2 * pairs:2].set(receiver + passed)
    return tallies[jax.random.permutation(jax.random.fold_in(own_key, 2), amount)]


def centred(rng, dims, deviation, bound, cuts=(), held_as=jnp.bfloat16):
    values = jax.random.normal(rng, dims, jnp.float32) * deviation
    if len(cuts) > 0:
        values = steps_of(rng, dims, cuts, -0.22, 0.18) * values
    return jnp.clip(values, min=-bound, max=bound).astype(held_as)


def setup_inputs(seed: int = 0) -> dict:
    splits = jax.random.split(jax.random.key(seed), 8)
    hidden = draw_hidden(jax.random.fold_in(splits[7], 71), 0)
    block_order = draw_block_order(jax.random.fold_in(splits[7], 71), 0)
    segment_ids = jnp.searchsorted(jnp.cumsum(ragged(splits[2], 4, TOKENS, TOKENS // 2, 0)), jnp.arange(TOKENS), side="right").astype(jnp.int32)
    w_query = centred(splits[3], (MODEL_WIDTH, QUERY_HEADS * HEAD_SIZE), MODEL_WIDTH ** -0.5, 0.09375, ((1, 4),))
    key_weight = centred(splits[4], (MODEL_WIDTH, KEY_VALUE_HEADS * HEAD_SIZE), MODEL_WIDTH ** -0.5, 0.09375, ((1, 4),))
    value_weight = centred(splits[5], (MODEL_WIDTH, KEY_VALUE_HEADS * HEAD_SIZE), MODEL_WIDTH ** -0.5, 0.09375, ((1, 4),))
    w_out = centred(splits[6], (QUERY_HEADS * HEAD_SIZE, MODEL_WIDTH), (QUERY_HEADS * HEAD_SIZE) ** -0.5, 0.09375, ((0, 4),))
    return {"hidden": hidden, "block_order": block_order, "segment_ids": segment_ids, "w_query": w_query, "key_weight": key_weight, "value_weight": value_weight, "w_out": w_out}


NEGATIVE_FILLER = -1e30
ROPE_BASE = 500000.0


def apply_rotary(values, block_places, heads):
    count_rows = values.shape[0]
    shaped = values.reshape(count_rows, heads, HEAD_SIZE)
    half_dim = HEAD_SIZE // 2
    freqs = ROPE_BASE ** (-(jnp.arange(half_dim, dtype=jnp.float32) * 2.0 / HEAD_SIZE))
    angles = block_places.astype(jnp.float32)[:, None] * freqs[None, :]
    cosine = jnp.cos(angles)[:, None, :]
    sine = jnp.sin(angles)[:, None, :]
    first_half = shaped[:, :, :half_dim]
    second_half = shaped[:, :, half_dim:]
    turned = jnp.concatenate([first_half * cosine - second_half * sine, second_half * cosine + first_half * sine], axis=2)
    return turned.reshape(count_rows, heads * HEAD_SIZE)


def attend(carry_state, query_matrix, query_pos, query_seg, key_block, value_block, key_pos, key_seg):
    running, totals, weighted = carry_state
    scores = jnp.einsum("qhgd,khd->hgqk", query_matrix.astype(jnp.float32), key_block.astype(jnp.float32)) * (HEAD_SIZE ** -0.5)
    allowed = (key_pos[None, :] <= query_pos[:, None]) & (key_seg[None, :] == query_seg[:, None])
    masked = jnp.where(allowed, scores, NEGATIVE_FILLER)
    newmax = jnp.maximum(running, jnp.max(masked, axis=3))
    expo = jnp.where(allowed, jnp.exp(scores - newmax[..., None]), 0.0)
    factor = jnp.exp(running - newmax)
    totals = totals * factor + jnp.sum(expo, axis=3)
    rounded = expo.astype(jnp.bfloat16).astype(jnp.float32)
    weighted = weighted * factor[..., None] + jnp.einsum("hgqk,khd->hgqd", rounded, value_block.astype(jnp.float32))
    return newmax, totals, weighted


def reference(hidden, block_order, segment_ids, w_query, key_weight, value_weight, w_out):
    inverse = jnp.zeros((NBLK,), jnp.int32).at[block_order].set(jnp.arange(NBLK, dtype=jnp.int32))
    sorted_blocks = hidden.reshape(NBLK, BLK, MODEL_WIDTH)[inverse].reshape(TOKENS, MODEL_WIDTH)
    block_places = jnp.arange(TOKENS, dtype=jnp.int32)
    query_matrix = apply_rotary(jnp.dot(sorted_blocks, w_query, preferred_element_type=jnp.float32), block_places, QUERY_HEADS).astype(jnp.bfloat16)
    every_key = apply_rotary(jnp.dot(sorted_blocks, key_weight, preferred_element_type=jnp.float32), block_places, KEY_VALUE_HEADS).astype(jnp.bfloat16)
    every_value = jnp.dot(sorted_blocks, value_weight, preferred_element_type=jnp.float32).astype(jnp.bfloat16)
    query_group = QUERY_HEADS // KEY_VALUE_HEADS
    query_block = math.gcd(512, TOKENS)
    nblocks = TOKENS // query_block

    def outer(index, outputs):
        starting_row = (index * query_block).astype(jnp.int32)
        query_rows = lax.dynamic_slice_in_dim(query_matrix, starting_row, query_block, 0).reshape(query_block, KEY_VALUE_HEADS, query_group, HEAD_SIZE)
        qpos = starting_row + jnp.arange(query_block, dtype=jnp.int32)
        qseg = lax.dynamic_slice_in_dim(segment_ids, starting_row, query_block, 0)
        start_state = (jnp.full((KEY_VALUE_HEADS, query_group, query_block), NEGATIVE_FILLER, jnp.float32),
                   jnp.zeros((KEY_VALUE_HEADS, query_group, query_block), jnp.float32),
                   jnp.zeros((KEY_VALUE_HEADS, query_group, query_block, HEAD_SIZE), jnp.float32))

        def inner_loop(key_index, carry_state):
            leading_key = (key_index * query_block).astype(jnp.int32)
            key_block = lax.dynamic_slice_in_dim(every_key, leading_key, query_block, 0).reshape(query_block, KEY_VALUE_HEADS, HEAD_SIZE)
            value_block = lax.dynamic_slice_in_dim(every_value, leading_key, query_block, 0).reshape(query_block, KEY_VALUE_HEADS, HEAD_SIZE)
            key_pos = leading_key + jnp.arange(query_block, dtype=jnp.int32)
            key_seg = lax.dynamic_slice_in_dim(segment_ids, leading_key, query_block, 0)
            return attend(carry_state, query_rows, qpos, qseg, key_block, value_block, key_pos, key_seg)

        finished = lax.fori_loop(0, index + 1, inner_loop, start_state)
        block_out = (finished[2] / finished[1][..., None]).transpose(2, 0, 1, 3).reshape(query_block, QUERY_HEADS * HEAD_SIZE)
        return lax.dynamic_update_slice_in_dim(outputs, block_out.astype(jnp.bfloat16), starting_row, 0)

    attended = lax.fori_loop(0, nblocks, outer, jnp.zeros((TOKENS, QUERY_HEADS * HEAD_SIZE), jnp.bfloat16))
    width = QUERY_HEADS * HEAD_SIZE // N_HEAD
    summed = jnp.zeros((TOKENS, MODEL_WIDTH), jnp.float32)
    for member in range(N_HEAD):
        partial_sum = jnp.dot(attended[:, member * width:(member + 1) * width], w_out[member * width:(member + 1) * width], preferred_element_type=jnp.float32)
        summed = summed + partial_sum.astype(jnp.bfloat16).astype(jnp.float32)
    result = summed.astype(jnp.bfloat16).reshape(NBLK, BLK, MODEL_WIDTH)[block_order].reshape(TOKENS, MODEL_WIDTH)
    return result
```

```python
import math

import jax
import jax.numpy as jnp
from jax import lax
from jax.experimental import pallas as pl
from jax.experimental.pallas import tpu as pltpu
from jax.sharding import PartitionSpec as P

HEAD_SIZE = 128


NEGATIVE_FILLER = -1e30
ROPE_BASE = 500000.0


def apply_rotary(values, block_places, heads):
    count_rows = values.shape[0]
    shaped = values.reshape(count_rows, heads, HEAD_SIZE)
    half_dim = HEAD_SIZE // 2
    freqs = ROPE_BASE ** (-(jnp.arange(half_dim, dtype=jnp.float32) * 2.0 / HEAD_SIZE))
    angles = block_places.astype(jnp.float32)[:, None] * freqs[None, :]
    cosine = jnp.cos(angles)[:, None, :]
    sine = jnp.sin(angles)[:, None, :]
    first_half = shaped[:, :, :half_dim]
    second_half = shaped[:, :, half_dim:]
    turned = jnp.concatenate(
        [first_half * cosine - second_half * sine, second_half * cosine + first_half * sine], axis=2
    )
    return turned.reshape(count_rows, heads * HEAD_SIZE)


def positions(stored_rows, order_table, block_len):
    which_block = stored_rows // block_len
    hits = which_block[:, None] == jnp.arange(order_table.shape[0], dtype=jnp.int32)[None, :]
    base = jnp.sum(jnp.where(hits, order_table[None, :], 0), axis=1)
    return base * block_len + stored_rows % block_len


def attend(
    carry_state, query_matrix, query_pos, query_seg, key_block, value_block, key_pos, key_seg
):
    running, totals, weighted = carry_state
    scores = jnp.einsum(
        "qhgd,khd->hgqk", query_matrix, key_block, preferred_element_type=jnp.float32
    ) * HEAD_SIZE ** (-0.5)
    allowed = (key_pos[None, :] <= query_pos[:, None]) & (key_seg[None, :] == query_seg[:, None])
    masked = jnp.where(allowed, scores, NEGATIVE_FILLER)
    newmax = jnp.maximum(running, jnp.max(masked, axis=3))
    expo = jnp.where(allowed, jnp.exp(scores - newmax[..., None]), 0.0)
    factor = jnp.exp(running - newmax)
    totals = totals * factor + jnp.sum(expo, axis=3)
    weighted = weighted * factor[..., None] + jnp.einsum(
        "hgqk,khd->hgqd", expo.astype(jnp.bfloat16), value_block, preferred_element_type=jnp.float32
    )
    return (newmax, totals, weighted)


def general_device(hidden, block_order, segment_ids, w_query, key_weight, value_weight, w_out):
    q_heads = w_query.shape[1] // HEAD_SIZE
    kv_heads = key_weight.shape[1] // HEAD_SIZE
    query_group = q_heads // kv_heads
    received = lax.all_gather(hidden, "head", axis=0, tiled=True)
    projected = jnp.concatenate(
        [
            jnp.dot(received, w_query, preferred_element_type=jnp.float32),
            jnp.dot(received, key_weight, preferred_element_type=jnp.float32),
            jnp.dot(received, value_weight, preferred_element_type=jnp.float32),
        ],
        axis=1,
    )
    local_rows = projected.shape[0]
    half_rows = local_rows // 2
    own_rows = lax.axis_index("seq") * local_rows + jnp.arange(local_rows, dtype=jnp.int32)
    own_pos = positions(own_rows, block_order, half_rows)
    own_seg = jnp.take(segment_ids, own_pos)
    query_matrix = (
        apply_rotary(projected[:, : q_heads * HEAD_SIZE], own_pos, q_heads)
        .astype(jnp.bfloat16)
        .reshape(local_rows, kv_heads, query_group, HEAD_SIZE)
    )
    keys_own = apply_rotary(
        projected[:, q_heads * HEAD_SIZE : (q_heads + kv_heads) * HEAD_SIZE], own_pos, kv_heads
    ).astype(jnp.bfloat16)
    values_own = projected[:, (q_heads + kv_heads) * HEAD_SIZE :].astype(jnp.bfloat16)
    start_state = (
        jnp.full((kv_heads, query_group, local_rows), NEGATIVE_FILLER, jnp.float32),
        jnp.zeros((kv_heads, query_group, local_rows), jnp.float32),
        jnp.zeros((kv_heads, query_group, local_rows, HEAD_SIZE), jnp.float32),
    )
    key_all, value_all = (
        lax.all_gather(keys_own, "seq", axis=0, tiled=True),
        lax.all_gather(values_own, "seq", axis=0, tiled=True),
    )
    count_rows = key_all.shape[0]
    key_rows = jnp.arange(count_rows, dtype=jnp.int32)
    key_pos = positions(key_rows, block_order, half_rows)
    key_seg = jnp.take(segment_ids, key_pos)
    step_len = math.gcd(count_rows, 4 * local_rows)
    steps_total = count_rows // step_len
    blocks = (
        key_all.reshape(steps_total, step_len, kv_heads, HEAD_SIZE),
        value_all.reshape(steps_total, step_len, kv_heads, HEAD_SIZE),
        key_pos.reshape(steps_total, step_len),
        key_seg.reshape(steps_total, step_len),
    )

    def visit(current, block_items):
        key_block, value_block, kpos_blk, kseg_blk = block_items
        updated = attend(
            current, query_matrix, own_pos, own_seg, key_block, value_block, kpos_blk, kseg_blk
        )
        return (updated, None)

    finished, unused = lax.scan(visit, start_state, blocks)
    running, totals, weighted = finished
    attended = (
        (weighted / totals[..., None])
        .transpose(2, 0, 1, 3)
        .reshape(local_rows, q_heads * HEAD_SIZE)
        .astype(jnp.bfloat16)
    )
    return lax.psum_scatter(
        jnp.dot(attended, w_out, preferred_element_type=jnp.float32).astype(jnp.bfloat16),
        "head",
        scatter_dimension=0,
        tiled=True,
    )


F32 = jnp.float32
BF16 = jnp.bfloat16


def turn(values, cosine, sine):
    return values * cosine + pltpu.roll(values, HEAD_SIZE // 2, 1) * sine


def kv_kernel(core_ref, own_ref, peer_ref, wk_ref, wv_ref, cos_ref, sin_ref, out_ref, acc_ref):
    step = pl.program_id(0)
    rows = own_ref.shape[0]
    width = wk_ref.shape[1]
    core = core_ref[0]
    first = jnp.where(core == 0, own_ref[...], peer_ref[...])
    second = jnp.where(core == 0, peer_ref[...], own_ref[...])
    both = jnp.concatenate([first, second], axis=0)

    @pl.when(step == 0)
    def _():
        acc_ref[...] = jnp.zeros_like(acc_ref)

    acc_ref[:, :width] += jnp.dot(both, wk_ref[...], preferred_element_type=F32)
    acc_ref[:, width:] += jnp.dot(both, wv_ref[...], preferred_element_type=F32)

    @pl.when(step == pl.num_programs(0) - 1)
    def _():
        for head in range(width // HEAD_SIZE):
            cut = slice(head * HEAD_SIZE, (head + 1) * HEAD_SIZE)
            out_ref[:, cut] = turn(acc_ref[:, cut], cos_ref[...], sin_ref[...]).astype(BF16)
        out_ref[:, width:] = acc_ref[:, width:].astype(BF16)


def project_kv(core, own, peer, wk, wv, cosine, sine):
    rows, depth = own.shape
    width = wk.shape[1]
    steps = 4
    part = depth // steps
    whole = lambda shape: pl.BlockSpec(shape, lambda k: (0, 0))
    return pl.pallas_call(
        kv_kernel,
        grid=(steps,),
        in_specs=[
            pl.BlockSpec(memory_space=pltpu.SMEM),
            pl.BlockSpec((rows, part), lambda k: (0, k)),
            pl.BlockSpec((rows, part), lambda k: (0, k)),
            pl.BlockSpec((part, width), lambda k: (k, 0)),
            pl.BlockSpec((part, width), lambda k: (k, 0)),
            whole(cosine.shape),
            whole(sine.shape),
        ],
        out_specs=whole((2 * rows, 2 * width)),
        out_shape=jax.ShapeDtypeStruct((2 * rows, 2 * width), BF16),
        scratch_shapes=[pltpu.VMEM((2 * rows, 2 * width), F32)],
        cost_estimate=pl.CostEstimate(
            flops=8 * rows * depth * width, bytes_accessed=4 * depth * width, transcendentals=0
        ),
        name="project_kv",
    )(core, own, peer, wk, wv, cosine, sine)


def q_kernel(core_ref, a_ref, b_ref, c_ref, d_ref, w_ref, cos_ref, sin_ref, out_ref, x_ref):
    rows = a_ref.shape[0]

    @pl.when(pl.program_id(0) == 0)
    def _():
        flip = core_ref[0] == 0
        for at, (own, peer) in enumerate(((a_ref, b_ref), (c_ref, d_ref))):
            base = 2 * rows * at
            x_ref[base : base + rows, :] = jnp.where(flip, own[...], peer[...])
            x_ref[base + rows : base + 2 * rows, :] = jnp.where(flip, peer[...], own[...])

    result = jnp.dot(x_ref[...], w_ref[...], preferred_element_type=F32)
    for head in range(w_ref.shape[1] // HEAD_SIZE):
        cut = slice(head * HEAD_SIZE, (head + 1) * HEAD_SIZE)
        out_ref[:, cut] = turn(result[:, cut], cos_ref[...], sin_ref[...]).astype(BF16)


def project_q(core, pieces, weight, cosine, sine):
    rows, depth = pieces[0].shape
    width = weight.shape[1]
    tile = 2 * HEAD_SIZE
    whole = lambda shape: pl.BlockSpec(shape, lambda n: (0, 0))
    return pl.pallas_call(
        q_kernel,
        grid=(width // tile,),
        in_specs=[pl.BlockSpec(memory_space=pltpu.SMEM)]
        + [whole(piece.shape) for piece in pieces]
        + [pl.BlockSpec((depth, tile), lambda n: (0, n)), whole(cosine.shape), whole(sine.shape)],
        out_specs=pl.BlockSpec((4 * rows, tile), lambda n: (0, n)),
        out_shape=jax.ShapeDtypeStruct((4 * rows, width), BF16),
        scratch_shapes=[pltpu.VMEM((4 * rows, depth), BF16)],
        cost_estimate=pl.CostEstimate(
            flops=8 * rows * depth * width, bytes_accessed=2 * depth * width, transcendentals=0
        ),
        name="project_q",
    )(core, *pieces, weight, cosine, sine)


def attention_kernel(
    info_ref, slot_ref, q_ref, qseg_ref, kseg_ref, *rest, pieces, block, kv_heads, group
):
    piece_refs = rest[:pieces]
    w_ref = rest[pieces]
    outs = rest[pieces + 1 : pieces + 5]
    w_vmem, kv_ref, qs_ref, s_ref, m_ref, l_ref, acc_ref, att_ref, sem = rest[pieces + 5 :]
    fetch = pltpu.make_async_copy(w_ref, w_vmem, sem)
    fetch.start()
    for at in range(pieces):
        kv_ref[at] = piece_refs[at][...]
    span = group * block
    width = kv_heads * HEAD_SIZE
    factor = HEAD_SIZE**-0.5 * math.log2(math.e)
    below = lax.broadcasted_iota(jnp.int32, (block, block), 1) <= lax.broadcasted_iota(
        jnp.int32, (block, block), 0
    )
    for at in range(2):
        low = info_ref[1 + 2 * at]
        high = info_ref[2 + 2 * at]
        row_cut = slice(at * block, (at + 1) * block)
        for head in range(kv_heads * group):
            qs_ref[head * block : (head + 1) * block, :] = q_ref[
                row_cut, head * HEAD_SIZE : (head + 1) * HEAD_SIZE
            ]
        m_ref[...] = jnp.full_like(m_ref, NEGATIVE_FILLER)
        l_ref[...] = jnp.zeros_like(l_ref)
        acc_ref[...] = jnp.zeros_like(acc_ref)
        qseg = qseg_ref[row_cut, :]

        def score(place, carry):
            slot = slot_ref[place]
            same = qseg == kseg_ref[pl.ds(place, 1), :]
            allowed = same & (below | (place < high))
            for kv in range(kv_heads):
                cut = slice(kv * span, (kv + 1) * span)
                scores = lax.dot_general(
                    qs_ref[cut, :],
                    kv_ref[slot, :, kv * HEAD_SIZE : (kv + 1) * HEAD_SIZE],
                    (((1,), (1,)), ((), ())),
                    preferred_element_type=F32,
                ).reshape(group, block, block)
                masked = jnp.where(allowed[None], scores, NEGATIVE_FILLER).reshape(span, block)
                s_ref[place, cut, :] = masked
                m_ref[cut, :] = jnp.maximum(m_ref[cut, :], masked)
            return carry

        lax.fori_loop(low, high + 1, score, 0)
        m_ref[...] = jnp.broadcast_to(jnp.max(m_ref[...], axis=1, keepdims=True), m_ref.shape)

        def weigh(place, carry):
            slot = slot_ref[place]
            for kv in range(kv_heads):
                cut = slice(kv * span, (kv + 1) * span)
                expo = jnp.exp2((s_ref[place, cut, :] - m_ref[cut, :]) * factor)
                l_ref[cut, :] += expo
                acc_ref[cut, :] += jnp.dot(
                    expo.astype(BF16),
                    kv_ref[slot, :, width + kv * HEAD_SIZE : width + (kv + 1) * HEAD_SIZE],
                    preferred_element_type=F32,
                )
            return carry

        lax.fori_loop(low, high + 1, weigh, 0)
        done = (acc_ref[...] / jnp.sum(l_ref[...], axis=1, keepdims=True)).astype(BF16)
        half = block // 2
        flip = info_ref[0] == 0
        for head in range(kv_heads * group):
            cut = slice(head * HEAD_SIZE, (head + 1) * HEAD_SIZE)
            base = head * block
            first, second = done[base : base + half], done[base + half : base + block]
            att_ref[2 * at * half : (2 * at + 1) * half, cut] = jnp.where(flip, first, second)
            att_ref[(2 * at + 1) * half : (2 * at + 2) * half, cut] = jnp.where(flip, second, first)
    fetch.wait()
    half = block // 2
    tile = w_vmem.shape[1] // 4
    for col in range(4):
        cut = slice(col * tile, (col + 1) * tile)
        partial = jnp.dot(att_ref[...], w_vmem[:, cut], preferred_element_type=F32).astype(BF16)
        for at in range(4):
            outs[at][:, cut] = partial[at * half : (at + 1) * half]


def attention_out(info, slots, queries, qseg, kseg, pieces, w_out, kv_heads, group):
    block = pieces[0].shape[0]
    count = len(pieces)
    tall = kv_heads * group * block
    vmem = pl.BlockSpec(memory_space=pltpu.VMEM)
    smem = pl.BlockSpec(memory_space=pltpu.SMEM)
    piece_out = jax.ShapeDtypeStruct((block // 2, w_out.shape[1]), BF16)
    kernel = lambda *refs: attention_kernel(
        *refs, pieces=count, block=block, kv_heads=kv_heads, group=group
    )
    return pl.pallas_call(
        kernel,
        in_specs=[smem, smem, vmem, vmem, vmem]
        + [vmem] * count
        + [pl.BlockSpec(memory_space=pl.ANY)],
        out_specs=[vmem] * 4,
        out_shape=[piece_out] * 4,
        scratch_shapes=[
            pltpu.VMEM(w_out.shape, BF16),
            pltpu.VMEM((count,) + pieces[0].shape, BF16),
            pltpu.VMEM((tall, HEAD_SIZE), BF16),
            pltpu.VMEM((count, tall, block), F32),
            pltpu.VMEM((tall, block), F32),
            pltpu.VMEM((tall, block), F32),
            pltpu.VMEM((tall, HEAD_SIZE), F32),
            pltpu.VMEM((2 * block, kv_heads * group * HEAD_SIZE), BF16),
            pltpu.SemaphoreType.DMA,
        ],
        cost_estimate=pl.CostEstimate(
            flops=8 * block * w_out.shape[0] * w_out.shape[1],
            bytes_accessed=2 * w_out.shape[0] * w_out.shape[1],
            transcendentals=0,
        ),
        name="attention_out",
    )(info, slots, queries, qseg, kseg, *pieces, w_out)


def rotary_tables(places):
    half_dim = HEAD_SIZE // 2
    freqs = ROPE_BASE ** (-(jnp.arange(half_dim, dtype=F32) * 2.0 / HEAD_SIZE))
    angles = places.astype(F32)[:, None] * freqs[None, :]
    cosine, sine = jnp.cos(angles), jnp.sin(angles)
    return jnp.concatenate([cosine, cosine], 1), jnp.concatenate([-sine, sine], 1)


def swap(values, axis, count, mask):
    return lax.ppermute(values, axis, [(at, at ^ mask) for at in range(count)])


def gather_seq(piece, shards, lanes):
    found = {0: piece}
    far = range(lanes, shards, lanes)
    for step in sorted(far, reverse=True):
        found[step] = swap(piece, "seq", shards, step)
    for step in [0] + list(far):
        for near in range(1, lanes):
            found[step + near] = swap(found[step], "seq", shards, near)
    return [found[step] for step in range(shards)]


def paired_device(shards, lanes):
    def on_device(hidden, block_order, segment_ids, w_query, key_weight, value_weight, w_out):
        blocks = block_order.shape[0]
        block = segment_ids.shape[0] // blocks
        kv_heads = key_weight.shape[1] // HEAD_SIZE
        group = w_query.shape[1] // key_weight.shape[1]
        shard = lax.axis_index("seq")
        place = lax.axis_index("head")
        core, chip = place % 2, place // 2
        across = swap(hidden, "head", 4, 2)
        beside = swap(hidden, "head", 4, 1)

        seg = segment_ids.reshape(blocks, block)
        steps = jnp.arange(shards, dtype=jnp.int32)
        stored = jnp.concatenate([2 * (shard ^ steps) + chip, 2 * (shard ^ steps) + 1 - chip])
        numbers = jnp.arange(blocks, dtype=jnp.int32)
        held = jnp.sum(
            jnp.where(stored[:, None] == numbers[None, :], block_order[None, :], 0), axis=1
        )
        slots = jnp.sum(
            jnp.where(held[None, :] == numbers[:, None], numbers[None, :], 0), axis=1
        )
        own = jnp.stack([held[0], held[shards]])
        mine = own[:, None] == numbers[None, :]
        qseg = jnp.sum(jnp.where(mine[:, :, None], seg[None], 0), axis=1)
        low = jnp.sum((seg[None, :, -1] < qseg[:, :1]).astype(jnp.int32), axis=1)
        info = jnp.stack([core, low[0], own[0], low[1], own[1]]).astype(jnp.int32)
        places = (own[:, None] * block + jnp.arange(block, dtype=jnp.int32)[None, :]).reshape(-1)
        cosine, sine = rotary_tables(places)
        qseg = jnp.broadcast_to(qseg.reshape(-1)[:, None], (2 * block, block))
        core_at = core.reshape(1).astype(jnp.int32)

        early = project_kv(
            core_at, hidden, beside, key_weight, value_weight, cosine[:block], sine[:block]
        )
        early_all = gather_seq(early, shards, lanes)
        across_beside = swap(across, "head", 4, 1)
        late = project_kv(
            core_at, across, across_beside, key_weight, value_weight, cosine[block:], sine[block:]
        )
        late_all = gather_seq(late, shards, lanes)
        queries = project_q(
            core_at, (hidden, beside, across, across_beside), w_query, cosine, sine
        )
        near_own, near_peer, far_own, far_peer = attention_out(
            info, slots, queries, qseg, seg, early_all + late_all, w_out, kv_heads, group
        )
        far_in = swap(far_peer, "head", 4, 1)
        near_in = swap(near_peer, "head", 4, 1)
        crossing = (far_own.astype(F32) + far_in.astype(F32)).astype(BF16)
        crossed = swap(crossing, "head", 4, 2)
        return (near_own.astype(F32) + near_in.astype(F32) + crossed.astype(F32)).astype(BF16)

    return on_device


def solution(mesh):
    placed = (
        P(("seq", "head"), None),
        P(),
        P(),
        P(None, "head"),
        P(None, "head"),
        P(None, "head"),
        P("head", None),
    )
    shards, members = mesh.shape["seq"], mesh.shape["head"]
    paired = members == 4 and shards & (shards - 1) == 0
    device = paired_device(shards, 1 << ((shards.bit_length() - 1) // 2)) if paired else general_device
    return jax.shard_map(
        device, mesh=mesh, in_specs=placed, out_specs=P(("seq", "head"), None), check_vma=False
    )
```

```python
import math

import jax
import jax.numpy as jnp
import numpy as np
from jax import lax
from jax.experimental import pallas as pl
from jax.experimental.pallas import tpu as pltpu
from jax.sharding import PartitionSpec as P

HEAD_SIZE = 128


NEGATIVE_FILLER = -1e30
ROPE_BASE = 500000.0


def apply_rotary(values, block_places, heads):
    count_rows = values.shape[0]
    shaped = values.reshape(count_rows, heads, HEAD_SIZE)
    half_dim = HEAD_SIZE // 2
    freqs = ROPE_BASE ** (-(jnp.arange(half_dim, dtype=jnp.float32) * 2.0 / HEAD_SIZE))
    angles = block_places.astype(jnp.float32)[:, None] * freqs[None, :]
    cosine = jnp.cos(angles)[:, None, :]
    sine = jnp.sin(angles)[:, None, :]
    first_half = shaped[:, :, :half_dim]
    second_half = shaped[:, :, half_dim:]
    turned = jnp.concatenate(
        [first_half * cosine - second_half * sine, second_half * cosine + first_half * sine], axis=2
    )
    return turned.reshape(count_rows, heads * HEAD_SIZE)


def positions(stored_rows, order_table, block_len):
    which_block = stored_rows // block_len
    hits = which_block[:, None] == jnp.arange(order_table.shape[0], dtype=jnp.int32)[None, :]
    base = jnp.sum(jnp.where(hits, order_table[None, :], 0), axis=1)
    return base * block_len + stored_rows % block_len


def attend(
    carry_state, query_matrix, query_pos, query_seg, key_block, value_block, key_pos, key_seg
):
    running, totals, weighted = carry_state
    scores = jnp.einsum(
        "qhgd,khd->hgqk", query_matrix, key_block, preferred_element_type=jnp.float32
    ) * HEAD_SIZE ** (-0.5)
    allowed = (key_pos[None, :] <= query_pos[:, None]) & (key_seg[None, :] == query_seg[:, None])
    masked = jnp.where(allowed, scores, NEGATIVE_FILLER)
    newmax = jnp.maximum(running, jnp.max(masked, axis=3))
    expo = jnp.where(allowed, jnp.exp(scores - newmax[..., None]), 0.0)
    factor = jnp.exp(running - newmax)
    totals = totals * factor + jnp.sum(expo, axis=3)
    weighted = weighted * factor[..., None] + jnp.einsum(
        "hgqk,khd->hgqd", expo.astype(jnp.bfloat16), value_block, preferred_element_type=jnp.float32
    )
    return (newmax, totals, weighted)


def general_device(hidden, block_order, segment_ids, w_query, key_weight, value_weight, w_out):
    q_heads = w_query.shape[1] // HEAD_SIZE
    kv_heads = key_weight.shape[1] // HEAD_SIZE
    query_group = q_heads // kv_heads
    received = lax.all_gather(hidden, "head", axis=0, tiled=True)
    projected = jnp.concatenate(
        [
            jnp.dot(received, w_query, preferred_element_type=jnp.float32),
            jnp.dot(received, key_weight, preferred_element_type=jnp.float32),
            jnp.dot(received, value_weight, preferred_element_type=jnp.float32),
        ],
        axis=1,
    )
    local_rows = projected.shape[0]
    half_rows = local_rows // 2
    own_rows = lax.axis_index("seq") * local_rows + jnp.arange(local_rows, dtype=jnp.int32)
    own_pos = positions(own_rows, block_order, half_rows)
    own_seg = jnp.take(segment_ids, own_pos)
    query_matrix = (
        apply_rotary(projected[:, : q_heads * HEAD_SIZE], own_pos, q_heads)
        .astype(jnp.bfloat16)
        .reshape(local_rows, kv_heads, query_group, HEAD_SIZE)
    )
    keys_own = apply_rotary(
        projected[:, q_heads * HEAD_SIZE : (q_heads + kv_heads) * HEAD_SIZE], own_pos, kv_heads
    ).astype(jnp.bfloat16)
    values_own = projected[:, (q_heads + kv_heads) * HEAD_SIZE :].astype(jnp.bfloat16)
    start_state = (
        jnp.full((kv_heads, query_group, local_rows), NEGATIVE_FILLER, jnp.float32),
        jnp.zeros((kv_heads, query_group, local_rows), jnp.float32),
        jnp.zeros((kv_heads, query_group, local_rows, HEAD_SIZE), jnp.float32),
    )
    key_all, value_all = (
        lax.all_gather(keys_own, "seq", axis=0, tiled=True),
        lax.all_gather(values_own, "seq", axis=0, tiled=True),
    )
    count_rows = key_all.shape[0]
    key_rows = jnp.arange(count_rows, dtype=jnp.int32)
    key_pos = positions(key_rows, block_order, half_rows)
    key_seg = jnp.take(segment_ids, key_pos)
    step_len = math.gcd(count_rows, 4 * local_rows)
    steps_total = count_rows // step_len
    blocks = (
        key_all.reshape(steps_total, step_len, kv_heads, HEAD_SIZE),
        value_all.reshape(steps_total, step_len, kv_heads, HEAD_SIZE),
        key_pos.reshape(steps_total, step_len),
        key_seg.reshape(steps_total, step_len),
    )

    def visit(current, block_items):
        key_block, value_block, kpos_blk, kseg_blk = block_items
        updated = attend(
            current, query_matrix, own_pos, own_seg, key_block, value_block, kpos_blk, kseg_blk
        )
        return (updated, None)

    finished, _ = lax.scan(visit, start_state, blocks)
    _, totals, weighted = finished
    attended = (
        (weighted / totals[..., None])
        .transpose(2, 0, 1, 3)
        .reshape(local_rows, q_heads * HEAD_SIZE)
        .astype(jnp.bfloat16)
    )
    return lax.psum_scatter(
        jnp.dot(attended, w_out, preferred_element_type=jnp.float32).astype(jnp.bfloat16),
        "head",
        scatter_dimension=0,
        tiled=True,
    )


F32 = jnp.float32
BF16 = jnp.bfloat16
ANY = pl.BlockSpec(memory_space=pl.ANY)
VMEM = pl.BlockSpec(memory_space=pltpu.VMEM)
SMEM = pl.BlockSpec(memory_space=pltpu.SMEM)


def frequencies():
    half_dim = HEAD_SIZE // 2
    freqs = ROPE_BASE ** (-(np.arange(half_dim) * 2.0 / HEAD_SIZE))
    return jnp.asarray(np.concatenate([freqs, freqs])[None, :].astype(np.float32))


def stored_block(far):
    chip = lax.axis_index("head") // 2
    return 2 * lax.axis_index("seq") + (1 - chip if far else chip)


def angles(number, freq_ref, block):
    rows = lax.broadcasted_iota(jnp.int32, (block, HEAD_SIZE), 0) + number * block
    turned = rows.astype(F32) * freq_ref[...]
    lane = lax.broadcasted_iota(jnp.int32, (block, HEAD_SIZE), 1)
    sine = jnp.sin(turned)
    return jnp.cos(turned), jnp.where(lane < HEAD_SIZE // 2, -sine, sine)


def turn(values, cosine, sine):
    return values * cosine + pltpu.roll(values, HEAD_SIZE // 2, 1) * sine


def start_rows(own_ref, peer_ref, x_ref, base, sems):
    rows = own_ref.shape[0]
    core = lax.axis_index("head") % 2
    copies = [
        pltpu.make_async_copy(own_ref, x_ref.at[pl.ds(base + core * rows, rows)], sems.at[0]),
        pltpu.make_async_copy(
            peer_ref, x_ref.at[pl.ds(base + (1 - core) * rows, rows)], sems.at[1]
        ),
    ]
    for copy in copies:
        copy.start()
    return copies


def kv_kernel(
    order_ref, freq_ref, own_ref, peer_ref, wk_ref, wv_ref, out_ref, x_ref, k_vmem, v_vmem, xs, ws, *, far
):
    rows, depth = own_ref.shape
    width = wk_ref.shape[1]
    parts = ws.shape[1]
    part = depth // parts
    x_copies = start_rows(own_ref, peer_ref, x_ref, 0, xs)
    copies = []
    for at in range(parts):
        cut = pl.ds(at * part, part)
        for which, (src, dst) in enumerate(((wk_ref, k_vmem), (wv_ref, v_vmem))):
            copy = pltpu.make_async_copy(src.at[cut], dst.at[cut], ws.at[which, at])
            copy.start()
            copies.append(copy)
    cosine, sine = angles(order_ref[stored_block(far)], freq_ref, 2 * rows)
    for copy in x_copies:
        copy.wait()
    keys = values = None
    for at in range(parts):
        copies[2 * at].wait()
        copies[2 * at + 1].wait()
        cut = slice(at * part, (at + 1) * part)
        more_k = jnp.dot(x_ref[:, cut], k_vmem[cut, :], preferred_element_type=F32)
        more_v = jnp.dot(x_ref[:, cut], v_vmem[cut, :], preferred_element_type=F32)
        keys = more_k if at == 0 else keys + more_k
        values = more_v if at == 0 else values + more_v
    for head in range(width // HEAD_SIZE):
        cut = slice(head * HEAD_SIZE, (head + 1) * HEAD_SIZE)
        out_ref[:, cut] = turn(keys[:, cut], cosine, sine).astype(BF16)
    out_ref[:, width:] = values.astype(BF16)


def project_kv(order, freqs, own, peer, wk, wv, far):
    rows, depth = own.shape
    width = wk.shape[1]
    parts = 4
    return pl.pallas_call(
        lambda *refs: kv_kernel(*refs, far=far),
        in_specs=[SMEM, VMEM, ANY, ANY, ANY, ANY],
        out_specs=VMEM,
        out_shape=jax.ShapeDtypeStruct((2 * rows, 2 * width), BF16),
        scratch_shapes=[
            pltpu.VMEM((2 * rows, depth), BF16),
            pltpu.VMEM((depth, width), BF16),
            pltpu.VMEM((depth, width), BF16),
            pltpu.SemaphoreType.DMA((2,)),
            pltpu.SemaphoreType.DMA((2, parts)),
        ],
        cost_estimate=pl.CostEstimate(
            flops=8 * rows * depth * width, bytes_accessed=4 * depth * width, transcendentals=0
        ),
        name="project_kv",
    )(order, freqs, own, peer, wk, wv)


def q_kernel(order_ref, freq_ref, own_ref, peer_ref, w_ref, out_ref, x_ref, w_vmem, xs, ws, *, far):
    rows = own_ref.shape[0]
    tiles, _, tile = w_vmem.shape
    x_copies = start_rows(own_ref, peer_ref, x_ref, 0, xs)
    copies = []
    for at in range(tiles):
        copy = pltpu.make_async_copy(
            w_ref.at[:, pl.ds(at * tile, tile)], w_vmem.at[at], ws.at[at]
        )
        copy.start()
        copies.append(copy)
    cosine, sine = angles(order_ref[stored_block(far)], freq_ref, 2 * rows)
    for copy in x_copies:
        copy.wait()
    for at in range(tiles):
        copies[at].wait()
        result = jnp.dot(x_ref[...], w_vmem[at], preferred_element_type=F32)
        for head in range(tile // HEAD_SIZE):
            cut = slice(head * HEAD_SIZE, (head + 1) * HEAD_SIZE)
            out_ref[:, at * tile + head * HEAD_SIZE : at * tile + (head + 1) * HEAD_SIZE] = turn(
                result[:, cut], cosine, sine
            ).astype(BF16)


def project_q(order, freqs, own, peer, weight, far):
    rows, depth = own.shape
    width = weight.shape[1]
    tile = 2 * HEAD_SIZE
    tiles = width // tile
    return pl.pallas_call(
        lambda *refs: q_kernel(*refs, far=far),
        in_specs=[SMEM, VMEM] + [ANY] * 3,
        out_specs=VMEM,
        out_shape=jax.ShapeDtypeStruct((2 * rows, width), BF16),
        scratch_shapes=[
            pltpu.VMEM((2 * rows, depth), BF16),
            pltpu.VMEM((tiles, depth, tile), BF16),
            pltpu.SemaphoreType.DMA((2,)),
            pltpu.SemaphoreType.DMA((tiles,)),
        ],
        cost_estimate=pl.CostEstimate(
            flops=4 * rows * depth * width, bytes_accessed=2 * depth * width, transcendentals=0
        ),
        name="project_q",
    )(order, freqs, own, peer, weight)


def attention_kernel(
    order_ref, seg_ref, segrow_ref, q_ref, *rest, pieces, block, kv_heads, group, far
):
    piece_refs = rest[:pieces]
    w_ref = rest[pieces]
    outs = rest[pieces + 1 : pieces + 3]
    w_vmem, kv_ref, qs_ref, s_ref, m_ref, l_ref, acc_ref, att_ref, slot_ref, ps, ws = rest[
        pieces + 3 :
    ]
    shards = pieces // 2
    chunks = ws.shape[0]
    chunk = w_ref.shape[0] // chunks
    copies = []
    for at in range(pieces):
        copies.append(pltpu.make_async_copy(piece_refs[at], kv_ref.at[at], ps.at[at]))
    fetch = [
        pltpu.make_async_copy(
            w_ref.at[pl.ds(at * chunk, chunk)], w_vmem.at[pl.ds(at * chunk, chunk)], ws.at[at]
        )
        for at in range(chunks)
    ]
    for copy in copies + fetch:
        copy.start()
    shard = lax.axis_index("seq")
    place = lax.axis_index("head")
    core, chip = place % 2, place // 2
    for at in range(shards):
        pair = 2 * (shard ^ at)
        slot_ref[order_ref[pair + chip]] = at
        slot_ref[order_ref[pair + 1 - chip]] = shards + at
    high = order_ref[stored_block(far)]
    leading = seg_ref[high * block]
    low = jnp.int32(0)
    for at in range(pieces):
        low = low + jnp.where(seg_ref[(at + 1) * block - 1] < leading, 1, 0)
    span = group * block
    width = kv_heads * HEAD_SIZE
    factor = HEAD_SIZE**-0.5 * math.log2(math.e)
    below = lax.broadcasted_iota(jnp.int32, (block, block), 1) <= lax.broadcasted_iota(
        jnp.int32, (block, block), 0
    )
    for head in range(kv_heads * group):
        qs_ref[head * block : (head + 1) * block, :] = q_ref[
            :, head * HEAD_SIZE : (head + 1) * HEAD_SIZE
        ]
    m_ref[...] = jnp.full_like(m_ref, NEGATIVE_FILLER)
    l_ref[...] = jnp.zeros_like(l_ref)
    acc_ref[...] = jnp.zeros_like(acc_ref)
    qseg = jnp.broadcast_to(segrow_ref[pl.ds(high, 1), :], (block, block)).T
    for copy in copies:
        copy.wait()

    def score(at, carry):
        slot = slot_ref[at]
        same = qseg == segrow_ref[pl.ds(at, 1), :]
        allowed = same & (below | (at < high))
        for kv in range(kv_heads):
            cut = slice(kv * span, (kv + 1) * span)
            scores = lax.dot_general(
                qs_ref[cut, :],
                kv_ref[slot, :, kv * HEAD_SIZE : (kv + 1) * HEAD_SIZE],
                (((1,), (1,)), ((), ())),
                preferred_element_type=F32,
            ).reshape(group, block, block)
            masked = jnp.where(allowed[None], scores, NEGATIVE_FILLER).reshape(span, block)
            s_ref[at, cut, :] = masked
            m_ref[cut, :] = jnp.maximum(m_ref[cut, :], masked)
        return carry

    lax.fori_loop(low, high + 1, score, 0)
    m_ref[...] = jnp.broadcast_to(jnp.max(m_ref[...], axis=1, keepdims=True), m_ref.shape)

    def weigh(at, carry):
        slot = slot_ref[at]
        for kv in range(kv_heads):
            cut = slice(kv * span, (kv + 1) * span)
            expo = jnp.exp2((s_ref[at, cut, :] - m_ref[cut, :]) * factor)
            l_ref[cut, :] += expo
            acc_ref[cut, :] += jnp.dot(
                expo.astype(BF16),
                kv_ref[slot, :, width + kv * HEAD_SIZE : width + (kv + 1) * HEAD_SIZE],
                preferred_element_type=F32,
            )
        return carry

    lax.fori_loop(low, high + 1, weigh, 0)
    done = (acc_ref[...] / jnp.sum(l_ref[...], axis=1, keepdims=True)).astype(BF16)
    half = block // 2
    flip = core == 0
    for head in range(kv_heads * group):
        cut = slice(head * HEAD_SIZE, (head + 1) * HEAD_SIZE)
        base = head * block
        first, second = done[base : base + half], done[base + half : base + block]
        att_ref[:half, cut] = jnp.where(flip, first, second)
        att_ref[half:, cut] = jnp.where(flip, second, first)
    for copy in fetch:
        copy.wait()
    tile = w_vmem.shape[1] // 4
    for col in range(4):
        cut = slice(col * tile, (col + 1) * tile)
        partial = jnp.dot(att_ref[...], w_vmem[:, cut], preferred_element_type=F32).astype(BF16)
        outs[0][:, cut] = partial[:half]
        outs[1][:, cut] = partial[half:]


def attention_out(order, segment_ids, seg_rows, queries, pieces, w_out, kv_heads, group, far):
    block = pieces[0].shape[0]
    count = len(pieces)
    tall = kv_heads * group * block
    chunks = 4
    piece_out = jax.ShapeDtypeStruct((block // 2, w_out.shape[1]), BF16)
    kernel = lambda *refs: attention_kernel(
        *refs, pieces=count, block=block, kv_heads=kv_heads, group=group, far=far
    )
    return pl.pallas_call(
        kernel,
        in_specs=[SMEM, SMEM, VMEM, VMEM] + [ANY] * (count + 1),
        out_specs=[VMEM] * 2,
        out_shape=[piece_out] * 2,
        scratch_shapes=[
            pltpu.VMEM(w_out.shape, BF16),
            pltpu.VMEM((count,) + pieces[0].shape, BF16),
            pltpu.VMEM((tall, HEAD_SIZE), BF16),
            pltpu.VMEM((count, tall, block), F32),
            pltpu.VMEM((tall, block), F32),
            pltpu.VMEM((tall, block), F32),
            pltpu.VMEM((tall, HEAD_SIZE), F32),
            pltpu.VMEM((block, kv_heads * group * HEAD_SIZE), BF16),
            pltpu.SMEM((count,), jnp.int32),
            pltpu.SemaphoreType.DMA((count,)),
            pltpu.SemaphoreType.DMA((chunks,)),
        ],
        cost_estimate=pl.CostEstimate(
            flops=4 * block * w_out.shape[0] * w_out.shape[1],
            bytes_accessed=2 * w_out.shape[0] * w_out.shape[1],
            transcendentals=0,
        ),
        name="attention_far" if far else "attention_near",
    )(order, segment_ids, seg_rows, queries, *pieces, w_out)


def swap(values, axis, count, mask):
    return lax.ppermute(values, axis, [(at, at ^ mask) for at in range(count)])


def gather_seq(piece, shards, lanes):
    found = {0: piece}
    far = range(lanes, shards, lanes)
    for step in sorted(far, reverse=True):
        found[step] = swap(piece, "seq", shards, step)
    for near in range(1, lanes):
        found[near] = swap(piece, "seq", shards, near)
    for step in far:
        for near in range(1, lanes):
            found[step + near] = swap(found[step], "seq", shards, near)
    return [found[step] for step in range(shards)]


def paired_device(shards, lanes):
    def on_device(hidden, order, segment_ids, w_query, key_weight, value_weight, w_out):
        return run(hidden, order, segment_ids, w_query, key_weight, value_weight, w_out)

    def run(hidden, order, segment_ids, w_query, key_weight, value_weight, w_out):
        seg_rows = segment_ids.reshape(order.shape[0], -1)
        kv_heads = key_weight.shape[1] // HEAD_SIZE
        group = w_query.shape[1] // key_weight.shape[1]
        freqs = frequencies()
        across = swap(hidden, "head", 4, 2)
        beside = swap(hidden, "head", 4, 1)
        early = project_kv(order, freqs, hidden, beside, key_weight, value_weight, False)
        early_all = gather_seq(early, shards, lanes)
        across_beside = swap(across, "head", 4, 1)
        late = project_kv(order, freqs, across, across_beside, key_weight, value_weight, True)
        late_all = gather_seq(late, shards, lanes)
        near_queries = project_q(order, freqs, hidden, beside, w_query, False)
        far_queries = project_q(order, freqs, across, across_beside, w_query, True)

        def attend_rows(q, far):
            return attention_out(
                order, segment_ids, seg_rows, q, early_all + late_all, w_out, kv_heads, group, far
            )

        far_own, far_peer = attend_rows(far_queries, True)
        far_in = swap(far_peer, "head", 4, 1)
        crossing = (far_own.astype(F32) + far_in.astype(F32)).astype(BF16)
        crossed = swap(crossing, "head", 4, 2)
        near_own, near_peer = attend_rows(near_queries, False)
        near_in = swap(near_peer, "head", 4, 1)
        return (near_own.astype(F32) + near_in.astype(F32) + crossed.astype(F32)).astype(BF16)

    return on_device


def solution(mesh):
    placed = (
        P(("seq", "head"), None),
        P(),
        P(),
        P(None, "head"),
        P(None, "head"),
        P(None, "head"),
        P("head", None),
    )
    shards, members = mesh.shape["seq"], mesh.shape["head"]
    paired = members == 4 and shards & (shards - 1) == 0
    device = paired_device(shards, 1 << ((shards.bit_length() - 1) // 2)) if paired else general_device
    return jax.shard_map(
        device, mesh=mesh, in_specs=placed, out_specs=P(("seq", "head"), None), check_vma=False
    )
```

```python
import math

import jax
import jax.numpy as jnp
import numpy as np
from jax import lax
from jax.experimental import pallas as pl
from jax.experimental.pallas import tpu as pltpu
from jax.sharding import PartitionSpec as P

HEAD_SIZE = 128


NEGATIVE_FILLER = -1e30
ROPE_BASE = 500000.0


def apply_rotary(values, block_places, heads):
    count_rows = values.shape[0]
    shaped = values.reshape(count_rows, heads, HEAD_SIZE)
    half_dim = HEAD_SIZE // 2
    freqs = ROPE_BASE ** (-(jnp.arange(half_dim, dtype=jnp.float32) * 2.0 / HEAD_SIZE))
    angles = block_places.astype(jnp.float32)[:, None] * freqs[None, :]
    cosine = jnp.cos(angles)[:, None, :]
    sine = jnp.sin(angles)[:, None, :]
    first_half = shaped[:, :, :half_dim]
    second_half = shaped[:, :, half_dim:]
    turned = jnp.concatenate(
        [first_half * cosine - second_half * sine, second_half * cosine + first_half * sine], axis=2
    )
    return turned.reshape(count_rows, heads * HEAD_SIZE)


def positions(stored_rows, order_table, block_len):
    which_block = stored_rows // block_len
    hits = which_block[:, None] == jnp.arange(order_table.shape[0], dtype=jnp.int32)[None, :]
    base = jnp.sum(jnp.where(hits, order_table[None, :], 0), axis=1)
    return base * block_len + stored_rows % block_len


def attend(
    carry_state, query_matrix, query_pos, query_seg, key_block, value_block, key_pos, key_seg
):
    running, totals, weighted = carry_state
    scores = jnp.einsum(
        "qhgd,khd->hgqk", query_matrix, key_block, preferred_element_type=jnp.float32
    ) * HEAD_SIZE ** (-0.5)
    allowed = (key_pos[None, :] <= query_pos[:, None]) & (key_seg[None, :] == query_seg[:, None])
    masked = jnp.where(allowed, scores, NEGATIVE_FILLER)
    newmax = jnp.maximum(running, jnp.max(masked, axis=3))
    expo = jnp.where(allowed, jnp.exp(scores - newmax[..., None]), 0.0)
    factor = jnp.exp(running - newmax)
    totals = totals * factor + jnp.sum(expo, axis=3)
    weighted = weighted * factor[..., None] + jnp.einsum(
        "hgqk,khd->hgqd", expo.astype(jnp.bfloat16), value_block, preferred_element_type=jnp.float32
    )
    return (newmax, totals, weighted)


def general_device(hidden, block_order, segment_ids, w_query, key_weight, value_weight, w_out):
    q_heads = w_query.shape[1] // HEAD_SIZE
    kv_heads = key_weight.shape[1] // HEAD_SIZE
    query_group = q_heads // kv_heads
    received = lax.all_gather(hidden, "head", axis=0, tiled=True)
    projected = jnp.concatenate(
        [
            jnp.dot(received, w_query, preferred_element_type=jnp.float32),
            jnp.dot(received, key_weight, preferred_element_type=jnp.float32),
            jnp.dot(received, value_weight, preferred_element_type=jnp.float32),
        ],
        axis=1,
    )
    local_rows = projected.shape[0]
    half_rows = local_rows // 2
    own_rows = lax.axis_index("seq") * local_rows + jnp.arange(local_rows, dtype=jnp.int32)
    own_pos = positions(own_rows, block_order, half_rows)
    own_seg = jnp.take(segment_ids, own_pos)
    query_matrix = (
        apply_rotary(projected[:, : q_heads * HEAD_SIZE], own_pos, q_heads)
        .astype(jnp.bfloat16)
        .reshape(local_rows, kv_heads, query_group, HEAD_SIZE)
    )
    keys_own = apply_rotary(
        projected[:, q_heads * HEAD_SIZE : (q_heads + kv_heads) * HEAD_SIZE], own_pos, kv_heads
    ).astype(jnp.bfloat16)
    values_own = projected[:, (q_heads + kv_heads) * HEAD_SIZE :].astype(jnp.bfloat16)
    start_state = (
        jnp.full((kv_heads, query_group, local_rows), NEGATIVE_FILLER, jnp.float32),
        jnp.zeros((kv_heads, query_group, local_rows), jnp.float32),
        jnp.zeros((kv_heads, query_group, local_rows, HEAD_SIZE), jnp.float32),
    )
    key_all, value_all = (
        lax.all_gather(keys_own, "seq", axis=0, tiled=True),
        lax.all_gather(values_own, "seq", axis=0, tiled=True),
    )
    count_rows = key_all.shape[0]
    key_rows = jnp.arange(count_rows, dtype=jnp.int32)
    key_pos = positions(key_rows, block_order, half_rows)
    key_seg = jnp.take(segment_ids, key_pos)
    step_len = math.gcd(count_rows, 4 * local_rows)
    steps_total = count_rows // step_len
    blocks = (
        key_all.reshape(steps_total, step_len, kv_heads, HEAD_SIZE),
        value_all.reshape(steps_total, step_len, kv_heads, HEAD_SIZE),
        key_pos.reshape(steps_total, step_len),
        key_seg.reshape(steps_total, step_len),
    )

    def visit(current, block_items):
        key_block, value_block, kpos_blk, kseg_blk = block_items
        updated = attend(
            current, query_matrix, own_pos, own_seg, key_block, value_block, kpos_blk, kseg_blk
        )
        return (updated, None)

    finished, _ = lax.scan(visit, start_state, blocks)
    _, totals, weighted = finished
    attended = (
        (weighted / totals[..., None])
        .transpose(2, 0, 1, 3)
        .reshape(local_rows, q_heads * HEAD_SIZE)
        .astype(jnp.bfloat16)
    )
    return lax.psum_scatter(
        jnp.dot(attended, w_out, preferred_element_type=jnp.float32).astype(jnp.bfloat16),
        "head",
        scatter_dimension=0,
        tiled=True,
    )


F32 = jnp.float32
BF16 = jnp.bfloat16
ANY = pl.BlockSpec(memory_space=pl.ANY)
VMEM = pl.BlockSpec(memory_space=pltpu.VMEM)
SMEM = pl.BlockSpec(memory_space=pltpu.SMEM)


def frequencies():
    half_dim = HEAD_SIZE // 2
    freqs = ROPE_BASE ** (-(np.arange(half_dim) * 2.0 / HEAD_SIZE))
    return jnp.asarray(np.concatenate([freqs, freqs])[None, :].astype(np.float32))


def stored_block(far):
    chip = lax.axis_index("head") // 2
    return 2 * lax.axis_index("seq") + (1 - chip if far else chip)


def angles(number, freq_ref, block):
    rows = lax.broadcasted_iota(jnp.int32, (block, HEAD_SIZE), 0) + number * block
    turned = rows.astype(F32) * freq_ref[...]
    lane = lax.broadcasted_iota(jnp.int32, (block, HEAD_SIZE), 1)
    sine = jnp.sin(turned)
    return jnp.cos(turned), jnp.where(lane < HEAD_SIZE // 2, -sine, sine)


def turn(values, cosine, sine):
    return values * cosine + pltpu.roll(values, HEAD_SIZE // 2, 1) * sine


def start_rows(own_ref, peer_ref, x_ref, base, sems):
    rows = own_ref.shape[0]
    core = lax.axis_index("head") % 2
    copies = [
        pltpu.make_async_copy(own_ref, x_ref.at[pl.ds(base + core * rows, rows)], sems.at[0]),
        pltpu.make_async_copy(
            peer_ref, x_ref.at[pl.ds(base + (1 - core) * rows, rows)], sems.at[1]
        ),
    ]
    for copy in copies:
        copy.start()
    return copies


def kv_kernel(
    first_ref, second_ref, own_ref, peer_ref, wk_ref, wv_ref, out_ref, x_ref, k_vmem, v_vmem, xs, ws, *, far
):
    rows, depth = own_ref.shape
    width = wk_ref.shape[1]
    parts = ws.shape[1]
    part = depth // parts
    x_copies = start_rows(own_ref, peer_ref, x_ref, 0, xs)
    copies = []
    for at in range(parts):
        cut = pl.ds(at * part, part)
        for which, (src, dst) in enumerate(((wk_ref, k_vmem), (wv_ref, v_vmem))):
            copy = pltpu.make_async_copy(src.at[cut], dst.at[cut], ws.at[which, at])
            copy.start()
            copies.append(copy)
    if far:
        cosine, sine = first_ref[...], second_ref[...]
    else:
        cosine, sine = angles(first_ref[stored_block(far)], second_ref, 2 * rows)
    for copy in x_copies:
        copy.wait()
    keys = values = None
    for at in range(parts):
        copies[2 * at].wait()
        copies[2 * at + 1].wait()
        cut = slice(at * part, (at + 1) * part)
        more_k = jnp.dot(x_ref[:, cut], k_vmem[cut, :], preferred_element_type=F32)
        more_v = jnp.dot(x_ref[:, cut], v_vmem[cut, :], preferred_element_type=F32)
        keys = more_k if at == 0 else keys + more_k
        values = more_v if at == 0 else values + more_v
    for head in range(width // HEAD_SIZE):
        cut = slice(head * HEAD_SIZE, (head + 1) * HEAD_SIZE)
        out_ref[:, cut] = turn(keys[:, cut], cosine, sine).astype(BF16)
    out_ref[:, width:] = values.astype(BF16)


def tables_kernel(order_ref, freq_ref, cos_ref, sin_ref):
    cos_ref[...], sin_ref[...] = angles(
        order_ref[stored_block(True)], freq_ref, cos_ref.shape[0]
    )


def rotary_tables(order, freqs, block):
    shape = jax.ShapeDtypeStruct((block, HEAD_SIZE), F32)
    return pl.pallas_call(
        tables_kernel,
        in_specs=[SMEM, VMEM],
        out_specs=[VMEM] * 2,
        out_shape=[shape] * 2,
        cost_estimate=pl.CostEstimate(
            flops=64 * block * HEAD_SIZE, bytes_accessed=8 * block * HEAD_SIZE, transcendentals=0
        ),
        name="rotary_tables",
    )(order, freqs)


def project_kv(first, second, own, peer, wk, wv, far):
    rows, depth = own.shape
    width = wk.shape[1]
    parts = 4
    return pl.pallas_call(
        lambda *refs: kv_kernel(*refs, far=far),
        in_specs=[VMEM if far else SMEM, VMEM, ANY, ANY, ANY, ANY],
        out_specs=VMEM,
        out_shape=jax.ShapeDtypeStruct((2 * rows, 2 * width), BF16),
        scratch_shapes=[
            pltpu.VMEM((2 * rows, depth), BF16),
            pltpu.VMEM((depth, width), BF16),
            pltpu.VMEM((depth, width), BF16),
            pltpu.SemaphoreType.DMA((2,)),
            pltpu.SemaphoreType.DMA((2, parts)),
        ],
        cost_estimate=pl.CostEstimate(
            flops=8 * rows * depth * width, bytes_accessed=4 * depth * width, transcendentals=0
        ),
        name="project_kv",
    )(first, second, own, peer, wk, wv)


def q_kernel(
    order_ref, freq_ref, cos_ref, sin_ref, a_ref, b_ref, c_ref, d_ref, w_ref, out_ref,
    x_ref, w_vmem, xs, ws,
):
    rows = a_ref.shape[0]
    tiles, _, tile = w_vmem.shape
    x_copies = start_rows(a_ref, b_ref, x_ref, 0, xs.at[0])
    x_copies += start_rows(c_ref, d_ref, x_ref, 2 * rows, xs.at[1])
    copies = []
    for at in range(tiles):
        copy = pltpu.make_async_copy(
            w_ref.at[:, pl.ds(at * tile, tile)], w_vmem.at[at], ws.at[at]
        )
        copy.start()
        copies.append(copy)
    cosine, sine = angles(order_ref[stored_block(False)], freq_ref, 2 * rows)
    cosine = jnp.concatenate([cosine, cos_ref[...]], axis=0)
    sine = jnp.concatenate([sine, sin_ref[...]], axis=0)
    for copy in x_copies:
        copy.wait()
    for at in range(tiles):
        copies[at].wait()
        result = jnp.dot(x_ref[...], w_vmem[at], preferred_element_type=F32)
        for head in range(tile // HEAD_SIZE):
            cut = slice(head * HEAD_SIZE, (head + 1) * HEAD_SIZE)
            out_ref[:, at * tile + head * HEAD_SIZE : at * tile + (head + 1) * HEAD_SIZE] = turn(
                result[:, cut], cosine, sine
            ).astype(BF16)


def project_q(order, freqs, tables, pieces, weight):
    rows, depth = pieces[0].shape
    width = weight.shape[1]
    tile = 2 * HEAD_SIZE
    tiles = width // tile
    return pl.pallas_call(
        q_kernel,
        in_specs=[SMEM, VMEM, VMEM, VMEM] + [ANY] * 5,
        out_specs=VMEM,
        out_shape=jax.ShapeDtypeStruct((4 * rows, width), BF16),
        scratch_shapes=[
            pltpu.VMEM((4 * rows, depth), BF16),
            pltpu.VMEM((tiles, depth, tile), BF16),
            pltpu.SemaphoreType.DMA((2, 2)),
            pltpu.SemaphoreType.DMA((tiles,)),
        ],
        cost_estimate=pl.CostEstimate(
            flops=8 * rows * depth * width, bytes_accessed=2 * depth * width, transcendentals=0
        ),
        name="project_q",
    )(order, freqs, *tables, *pieces, weight)


def attention_kernel(
    order_ref, seg_ref, segrow_ref, q_ref, *rest, pieces, block, kv_heads, group, far
):
    piece_refs = rest[:pieces]
    w_ref = rest[pieces]
    outs = rest[pieces + 1 : pieces + 3]
    w_vmem, kv_ref, qs_ref, s_ref, m_ref, l_ref, acc_ref, att_ref, slot_ref, ps, ws = rest[
        pieces + 3 :
    ]
    shards = pieces // 2
    chunks = ws.shape[0]
    chunk = w_ref.shape[0] // chunks
    copies = []
    for at in range(pieces):
        copies.append(pltpu.make_async_copy(piece_refs[at], kv_ref.at[at], ps.at[at]))
    fetch = [
        pltpu.make_async_copy(
            w_ref.at[pl.ds(at * chunk, chunk)], w_vmem.at[pl.ds(at * chunk, chunk)], ws.at[at]
        )
        for at in range(chunks)
    ]
    for copy in copies + fetch:
        copy.start()
    shard = lax.axis_index("seq")
    place = lax.axis_index("head")
    core, chip = place % 2, place // 2
    for at in range(shards):
        pair = 2 * (shard ^ at)
        slot_ref[order_ref[pair + chip]] = at
        slot_ref[order_ref[pair + 1 - chip]] = shards + at
    high = order_ref[stored_block(far)]
    leading = seg_ref[high * block]
    low = jnp.int32(0)
    for at in range(pieces):
        low = low + jnp.where(seg_ref[(at + 1) * block - 1] < leading, 1, 0)
    span = group * block
    width = kv_heads * HEAD_SIZE
    factor = HEAD_SIZE**-0.5 * math.log2(math.e)
    below = lax.broadcasted_iota(jnp.int32, (block, block), 1) <= lax.broadcasted_iota(
        jnp.int32, (block, block), 0
    )
    for head in range(kv_heads * group):
        qs_ref[head * block : (head + 1) * block, :] = q_ref[
            block * far : block * (far + 1), head * HEAD_SIZE : (head + 1) * HEAD_SIZE
        ]
    m_ref[...] = jnp.full_like(m_ref, NEGATIVE_FILLER)
    l_ref[...] = jnp.zeros_like(l_ref)
    acc_ref[...] = jnp.zeros_like(acc_ref)
    qseg = jnp.broadcast_to(segrow_ref[pl.ds(high, 1), :], (block, block)).T
    for copy in copies:
        copy.wait()

    def score(at, carry):
        slot = slot_ref[at]
        same = qseg == segrow_ref[pl.ds(at, 1), :]
        allowed = same & (below | (at < high))
        for kv in range(kv_heads):
            cut = slice(kv * span, (kv + 1) * span)
            scores = lax.dot_general(
                qs_ref[cut, :],
                kv_ref[slot, :, kv * HEAD_SIZE : (kv + 1) * HEAD_SIZE],
                (((1,), (1,)), ((), ())),
                preferred_element_type=F32,
            ).reshape(group, block, block)
            masked = jnp.where(allowed[None], scores, NEGATIVE_FILLER).reshape(span, block)
            s_ref[at, cut, :] = masked
            m_ref[cut, :] = jnp.maximum(m_ref[cut, :], masked)
        return carry

    lax.fori_loop(low, high + 1, score, 0)
    m_ref[...] = jnp.broadcast_to(jnp.max(m_ref[...], axis=1, keepdims=True), m_ref.shape)

    def weigh(at, carry):
        slot = slot_ref[at]
        for kv in range(kv_heads):
            cut = slice(kv * span, (kv + 1) * span)
            expo = jnp.exp2((s_ref[at, cut, :] - m_ref[cut, :]) * factor)
            l_ref[cut, :] += expo
            acc_ref[cut, :] += jnp.dot(
                expo.astype(BF16),
                kv_ref[slot, :, width + kv * HEAD_SIZE : width + (kv + 1) * HEAD_SIZE],
                preferred_element_type=F32,
            )
        return carry

    lax.fori_loop(low, high + 1, weigh, 0)
    done = (acc_ref[...] / jnp.sum(l_ref[...], axis=1, keepdims=True)).astype(BF16)
    half = block // 2
    flip = core == 0
    for head in range(kv_heads * group):
        cut = slice(head * HEAD_SIZE, (head + 1) * HEAD_SIZE)
        base = head * block
        first, second = done[base : base + half], done[base + half : base + block]
        att_ref[:half, cut] = jnp.where(flip, first, second)
        att_ref[half:, cut] = jnp.where(flip, second, first)
    for copy in fetch:
        copy.wait()
    tile = w_vmem.shape[1] // 4
    for col in range(4):
        cut = slice(col * tile, (col + 1) * tile)
        partial = jnp.dot(att_ref[...], w_vmem[:, cut], preferred_element_type=F32).astype(BF16)
        outs[0][:, cut] = partial[:half]
        outs[1][:, cut] = partial[half:]


def attention_out(order, segment_ids, seg_rows, queries, pieces, w_out, kv_heads, group, far):
    block = pieces[0].shape[0]
    count = len(pieces)
    tall = kv_heads * group * block
    chunks = 4
    piece_out = jax.ShapeDtypeStruct((block // 2, w_out.shape[1]), BF16)
    kernel = lambda *refs: attention_kernel(
        *refs, pieces=count, block=block, kv_heads=kv_heads, group=group, far=far
    )
    return pl.pallas_call(
        kernel,
        in_specs=[SMEM, SMEM, VMEM, VMEM] + [ANY] * (count + 1),
        out_specs=[VMEM] * 2,
        out_shape=[piece_out] * 2,
        scratch_shapes=[
            pltpu.VMEM(w_out.shape, BF16),
            pltpu.VMEM((count,) + pieces[0].shape, BF16),
            pltpu.VMEM((tall, HEAD_SIZE), BF16),
            pltpu.VMEM((count, tall, block), F32),
            pltpu.VMEM((tall, block), F32),
            pltpu.VMEM((tall, block), F32),
            pltpu.VMEM((tall, HEAD_SIZE), F32),
            pltpu.VMEM((block, kv_heads * group * HEAD_SIZE), BF16),
            pltpu.SMEM((count,), jnp.int32),
            pltpu.SemaphoreType.DMA((count,)),
            pltpu.SemaphoreType.DMA((chunks,)),
        ],
        cost_estimate=pl.CostEstimate(
            flops=4 * block * w_out.shape[0] * w_out.shape[1],
            bytes_accessed=2 * w_out.shape[0] * w_out.shape[1],
            transcendentals=0,
        ),
        name="attention_far" if far else "attention_near",
    )(order, segment_ids, seg_rows, queries, *pieces, w_out)


def swap(values, axis, count, mask):
    return lax.ppermute(values, axis, [(at, at ^ mask) for at in range(count)])


def gather_seq(piece, shards, lanes):
    found = {0: piece}
    far = range(lanes, shards, lanes)
    for near in range(1, lanes):
        found[near] = swap(piece, "seq", shards, near)
    for step in sorted(far, reverse=True):
        found[step] = swap(piece, "seq", shards, step)
    for step in far:
        for near in range(1, lanes):
            if step == lanes:
                found[step + near] = swap(found[near], "seq", shards, step)
            else:
                found[step + near] = swap(found[step], "seq", shards, near)
    return [found[step] for step in range(shards)]


def paired_device(shards, lanes):
    def on_device(hidden, order, segment_ids, w_query, key_weight, value_weight, w_out):
        return run(hidden, order, segment_ids, w_query, key_weight, value_weight, w_out)

    def run(hidden, order, segment_ids, w_query, key_weight, value_weight, w_out):
        seg_rows = segment_ids.reshape(order.shape[0], -1)
        kv_heads = key_weight.shape[1] // HEAD_SIZE
        group = w_query.shape[1] // key_weight.shape[1]
        freqs = frequencies()
        across = swap(hidden, "head", 4, 2)
        beside = swap(hidden, "head", 4, 1)
        tables = rotary_tables(order, freqs, seg_rows.shape[1])
        early = project_kv(order, freqs, hidden, beside, key_weight, value_weight, False)
        early_all = gather_seq(early, shards, lanes)
        across_beside = swap(across, "head", 4, 1)
        late = project_kv(*tables, across, across_beside, key_weight, value_weight, True)
        late_all = gather_seq(late, shards, lanes)
        queries = project_q(
            order, freqs, tables, (hidden, beside, across, across_beside), w_query
        )

        def attend_rows(q, far):
            return attention_out(
                order, segment_ids, seg_rows, q, early_all + late_all, w_out, kv_heads, group, far
            )

        far_own, far_peer = attend_rows(queries, True)
        far_in = swap(far_peer, "head", 4, 1)
        crossing = (far_own.astype(F32) + far_in.astype(F32)).astype(BF16)
        crossed = swap(crossing, "head", 4, 2)
        near_own, near_peer = attend_rows(queries, False)
        near_in = swap(near_peer, "head", 4, 1)
        return (near_own.astype(F32) + near_in.astype(F32) + crossed.astype(F32)).astype(BF16)

    return on_device


def solution(mesh):
    placed = (
        P(("seq", "head"), None),
        P(),
        P(),
        P(None, "head"),
        P(None, "head"),
        P(None, "head"),
        P("head", None),
    )
    shards, members = mesh.shape["seq"], mesh.shape["head"]
    paired = members == 4 and shards & (shards - 1) == 0
    device = paired_device(shards, 1 << ((shards.bit_length() - 1) // 2)) if paired else general_device
    return jax.shard_map(
        device, mesh=mesh, in_specs=placed, out_specs=P(("seq", "head"), None), check_vma=False
    )
```
